512 devices in a mesh: grp: 64 (over z, x_lo, core), tp: 8 (over x_hi, y).
Axes of the slice: x: 4 (x_hi: 2, x_lo: 2; x = x_hi * 2 + x_lo), y: 4, z: 16, core: 2. Of those that a mesh axis runs over, the one named last changes fastest.
Arguments:
- memory_rows: bfloat16 [65536, 4096], P('grp', 'tp'), may hold values from -24 to 24, as said below
- norm_gain: float32 [4096], replicated, may hold values from 0.25 to 1.75
- key_weight: bfloat16 [4096, 4096], P(None, 'tp'), may hold values from -0.09375 to 0.09375
- owner_table: int32 [8192], replicated, may hold values from 0 to 8191, as said below
Outputs:
- placed_keys: bfloat16 [65536, 4096], P('grp', 'tp')
The draws below stay inside these ranges and needn't reach their ends.
Inputs may be any that keep to these rules, and one draw needn't show every extreme that they name: A permutation of the 8192 block numbers. Block b of the input goes to block position owner_table[b], which lies in group owner_table[b] // 128. The 128 blocks of one group go to all 64 groups, exactly 2 blocks to each of them. `memory_rows`: rows have offsets and scales of their own, and features a common pattern.
All inputs are finite; a program needn't handle non-finite values.
Results may differ from the reference program's by a relative error of at most 0.0049.
Values may be sent and summed in bfloat16 or wider, within the bound.
A program may use at most 64 MiB of HBM per device.

```python
import jax
import jax.numpy as jnp
from jax import lax

D = 4096
BLK_ROWS = 8
BLK_DEV = 128
ROWS = 65536
NB = 8192


def draw_memory_rows(key, part):
    key_off, key_scale, key_noise, key_pattern = jax.random.split(key, 4)
    offsets = jax.random.uniform(key_off, (ROWS, 1), jnp.float32, -1.5, 1.5)
    pattern = jnp.clip(jax.random.normal(key_pattern, (1, D), jnp.float32), -3.0, 3.0)
    scales = jnp.exp(jax.random.uniform(key_scale, (ROWS, 1), jnp.float32, jnp.log(0.5), jnp.log(3.0)))
    noise = jnp.clip(jax.random.normal(key_noise, (ROWS, D), jnp.float32), -4.0, 4.0)
    values = offsets + scales * (noise + 0.7 * pattern)
    return jnp.clip(values, -24.0, 24.0).astype(jnp.bfloat16)


def draw_owner_table(key, part):
    groups = NB // BLK_DEV
    per_pair = BLK_DEV // groups
    key_tau, key_offs, key_cols, key_slots = jax.random.split(key, 4)
    shuffle = jax.random.permutation(key_tau, groups).astype(jnp.int32)
    offsets = jax.random.permutation(key_offs, groups).astype(jnp.int32)
    column_keys = jax.random.split(key_cols, groups)
    column_perm = jax.vmap(lambda one_key: jax.random.permutation(one_key, BLK_DEV))(column_keys).astype(jnp.int32)
    sources = jnp.arange(groups, dtype=jnp.int32)[:, None]
    target = shuffle[(sources + offsets[column_perm % groups]) % groups]
    arrival = sources * per_pair + column_perm // groups
    slot_keys = jax.random.split(key_slots, groups)
    slot_perm = jax.vmap(lambda one_key: jax.random.permutation(one_key, BLK_DEV))(slot_keys).astype(jnp.int32)
    slots = slot_perm[target, arrival]
    return (target * BLK_DEV + slots).reshape(-1).astype(jnp.int32)


def level_of(own_key, extent, cuts, low, high):
    def one(axis_at, blocks):
        draws = jax.random.uniform(jax.random.fold_in(jax.random.fold_in(own_key, 6), axis_at), (blocks,), jnp.float32, low / len(cuts), high / len(cuts))
        return jnp.repeat(jnp.exp(draws), extent[axis_at] // blocks).reshape((-1,) + (1,) * (len(extent) - axis_at - 1))

    factor_of = one(*cuts[0])
    for cut in cuts[1:]:
        factor_of = factor_of * one(*cut)
    return factor_of


def normal_values(rng, dims, width, reach, cuts=(), kind=jnp.bfloat16):
    values = jax.random.normal(rng, dims, jnp.float32) * width
    if len(cuts) > 0:
        values = level_of(rng, dims, cuts, -0.22, 0.18) * values
    return jnp.clip(values, min=-reach, max=reach).astype(kind)


def setup_inputs(seed: int = 0) -> dict:
    arg_keys = jax.random.split(jax.random.key(seed), 5)
    memory_rows = draw_memory_rows(jax.random.fold_in(arg_keys[4], 71), 0)
    norm_gain = jnp.clip(1.0 + 0.15 * jax.random.normal(arg_keys[1], (D,), jnp.float32), 0.25, 1.75)
    key_weight = normal_values(arg_keys[2], (D, D), D ** -0.5, 0.09375, ((1, 8),))
    owner_table = draw_owner_table(jax.random.fold_in(arg_keys[4], 71), 0)
    return dict(memory_rows=memory_rows, norm_gain=norm_gain, key_weight=key_weight, owner_table=owner_table)


EPS = 1e-05

def reference(memory_rows, norm_gain, key_weight, owner_table):
    values = memory_rows.astype(jnp.float32)
    row_sum = lax.optimization_barrier(jnp.sum(values, axis=1, keepdims=True))
    row_sq = lax.optimization_barrier(jnp.sum(values * values, axis=1, keepdims=True))
    row_mean = row_sum / D
    row_var = row_sq / D - row_mean * row_mean
    normed = ((values - row_mean) * lax.rsqrt(row_var + EPS) * norm_gain[None, :]).astype(jnp.bfloat16)
    keys = jnp.dot(normed, key_weight, preferred_element_type=jnp.float32).astype(jnp.bfloat16)
    blocks = keys.reshape(NB, BLK_ROWS, D)
    placed = jnp.zeros_like(blocks).at[owner_table.astype(jnp.int32)].set(blocks)
    return placed.reshape(ROWS, D)
```

```python
import functools

import jax
import jax.numpy as jnp
from jax import lax
from jax.experimental import pallas as pl
from jax.experimental.pallas import tpu as pltpu
from jax.sharding import PartitionSpec as P

BLK_ROWS = 8
EPS = 1e-05
MIB = 1024 * 1024
MESH = pl.DeviceIdType.MESH

NZ = 16
NY = 4
NX = 4
PER_Z = 4
CHUNKS = 8
PIECES = 8
FIRST_OTHER = 5


def shift_of(i, e):
    odd = i % 2
    half = i // 2
    d = (1 - odd) * (half + 1) + odd * (7 - half) - 4 * (i // 7)
    return d + e * (NZ - 2 * d - 8 * (i // 7))


def core_served(x):
    return ((x + 1) // 2 + 1) % 2


def index_kernel(groups, table_ref, slot_ref, index_ref):
    me = lax.axis_index("grp")
    blocks = table_ref.shape[1]
    capacity = blocks // groups
    lane = lax.broadcasted_iota(jnp.int32, (groups, blocks), 1)
    row = lax.broadcasted_iota(jnp.int32, (groups, blocks), 0)

    def ranked(offset, value):
        chosen = (offset >= 0) & (offset < blocks)
        counted = chosen.astype(jnp.int32)
        shift = 1
        while shift < blocks:
            counted = counted + jnp.where(lane >= shift, pltpu.roll(counted, shift, 1), 0)
            shift *= 2
        result = jnp.zeros((groups, blocks), jnp.int32)
        for r in range(capacity):
            at_rank = jnp.where(chosen & (counted == r + 1), value, 0).astype(jnp.float32)
            found = jnp.sum(at_rank, axis=1, keepdims=True).astype(jnp.int32)
            result = jnp.where(lane == r, found, result)
        return result

    own = jnp.broadcast_to(table_ref[pl.ds(me, 1), :], (groups, blocks))
    index_ref[...] = ranked(own - row * blocks, lane)
    offset = table_ref[...] - me * blocks
    slot_ref[...] = ranked(offset, offset)


def place_kernel(slot_ref, in_ref, out_ref, sem):
    z = lax.axis_index("grp") // PER_Z
    blocks = in_ref.shape[0]

    def move(n, carry):
        s = n // (blocks // 2)
        i = (n // 8) % CHUNKS
        e = (n // 4) % 2
        a = (n // 2) % 2
        source = ((z - shift_of(i, e) + NZ) % NZ) * PER_Z + a * 2 + s
        slot = slot_ref[source, n % 2]
        pltpu.make_async_copy(in_ref.at[n], out_ref.at[slot], sem).start()
        return carry

    lax.fori_loop(0, blocks, move, 0, unroll=8)
    pltpu.make_async_copy(in_ref, out_ref, sem).wait()


def main_kernel(
    index_ref, rows_ref, gain_ref, weight_ref, out_ref,
    raw, away, gath, weight, other, keys, normed, gains,
    raw_sem, weight_sem, gain_sem, z_send, z_recv, y_send, y_recv, f_send, f_recv,
    b_send, b_recv, a_send, a_recv, c_send, c_recv, k_send, k_recv,
):
    g = lax.axis_index("grp")
    t = lax.axis_index("tp")
    z = g // PER_Z
    x_lo = (g // 2) % 2
    core = g % 2
    x_hi = t // NY
    y = t % NY
    x = x_lo + 2 * x_hi
    served = core_served(x)
    keeps = 1 - (served + core) % 2
    depth = rows_ref.shape[2]
    width = weight_ref.shape[0]
    parts = width // depth
    chunk = 8 * BLK_ROWS
    half = CHUNKS * chunk
    quarter = width // 4
    piece = quarter // PIECES

    a_peer = {"grp": g + 2 * (1 - 2 * x_lo), "tp": t}
    b_peer = {"grp": g + 2 * (1 - 2 * x_lo), "tp": t + NY * (1 - 2 * x_hi)}
    c_peer = {"grp": g + 1 - 2 * core, "tp": t}
    up = {"grp": g, "tp": x_hi * NY + (y + 1) % NY}
    down = {"grp": g, "tp": x_hi * NY + (y + NY - 1) % NY}

    barrier = pltpu.get_barrier_semaphore()
    for peer in (a_peer, b_peer, c_peer, up, down):
        pl.semaphore_signal(barrier, inc=1, device_id=peer, device_id_type=MESH)

    def greet(n, carry):
        zs = (z + n // NX) % NZ
        xs = (x + n) % NX

        @pl.when(n + 1 - keeps > 0)
        def _():
            pl.semaphore_signal(
                barrier, inc=1,
                device_id={"grp": zs * PER_Z + (xs % 2) * 2 + served, "tp": (xs // 2) * NY + y},
                device_id_type=MESH,
            )

        return carry

    lax.fori_loop(0, NZ * NX, greet, 0)

    raw_copy = pltpu.make_async_copy(rows_ref, raw, raw_sem)
    raw_copy.start()

    def origin(j):
        r, h = j // 2, j % 2
        return h * NY + (y + (0, NY - 1, 1, 2)[r]) % NY

    def weight_copy(j):
        return pltpu.make_async_copy(
            weight_ref.at[pl.ds(pl.multiple_of(origin(j) * depth, depth), depth)],
            weight.at[pl.ds(j * depth, depth)],
            weight_sem.at[j],
        )

    def gain_copy(j):
        return pltpu.make_async_copy(
            gain_ref.at[:, pl.ds(pl.multiple_of(origin(j) * depth, depth), depth)],
            gains.at[:, pl.ds(j * depth, depth)],
            gain_sem.at[j],
        )

    for j in range(parts):
        gain_copy(j).start()
    for j in range(parts):
        weight_copy(j).start()

    def self_step(i, n):
        e, xl, k = n // 4, (n // 2) % 2, n % 2
        differs = (xl + x_lo + 1) % 2 + (k + core) % 2
        return keeps * (i // (CHUNKS - 1)) * (1 - e) * (1 - (differs + 1) // 2)

    def self_source(i, m):
        h, e, a = m // 4, (m // 2) % 2, m % 2
        differs = (h + x_hi) % 2 + (a + x_lo) % 2
        return keeps * (i // (CHUNKS - 1)) * (1 - e) * (1 - (differs + 1) // 2)

    def z_copy(i, n):
        e, xl, k = n // 4, (n // 2) % 2, n % 2
        to_z = (z + shift_of(i, e)) % NZ
        c = (xl + 1 + 2 * core) % NX
        return pltpu.make_async_remote_copy(
            src_ref=away.at[i * 8 + n],
            dst_ref=gath.at[0, i, x_hi, pl.ds((e * 2 + x_lo) * 2, 2)],
            send_sem=z_send.at[i * 8 + n],
            recv_sem=z_recv.at[i * 8 + x_hi * 4 + e * 2 + x_lo],
            device_id={"grp": to_z * PER_Z + (c % 2) * 2 + k, "tp": (c // 2) * NY + y},
            device_id_type=MESH,
        )

    def z_arrival(i, m):
        h, e, a = m // 4, (m // 2) % 2, m % 2
        return pltpu.make_async_remote_copy(
            src_ref=away.at[i * 8 + m],
            dst_ref=gath.at[0, i, h, pl.ds((e * 2 + a) * 2, 2)],
            send_sem=z_send.at[i * 8 + m],
            recv_sem=z_recv.at[i * 8 + m],
            device_id=a_peer,
            device_id_type=MESH,
        )

    def y_copy(i, way):
        return pltpu.make_async_remote_copy(
            src_ref=gath.at[0, i],
            dst_ref=gath.at[1 + way, i],
            send_sem=y_send.at[way, i],
            recv_sem=y_recv.at[way, i],
            device_id=(up, down)[way],
            device_id_type=MESH,
        )

    def f_copy(i, way):
        return pltpu.make_async_remote_copy(
            src_ref=gath.at[1 + way, i, way],
            dst_ref=gath.at[3, i, way],
            send_sem=f_send.at[way, i],
            recv_sem=f_recv.at[way, i],
            device_id=(up, down)[way],
            device_id_type=MESH,
        )

    def piece_of(q, p):
        return pl.ds(pl.multiple_of(q * quarter + p * piece, piece), piece)

    def b_copy(p):
        at = piece_of((1 - x_lo) * 2 + core, p)
        return pltpu.make_async_remote_copy(
            src_ref=weight.at[at], dst_ref=other.at[at],
            send_sem=b_send.at[p], recv_sem=b_recv.at[p],
            device_id=b_peer, device_id_type=MESH,
        )

    def a_copy(p):
        at = piece_of(x_lo * 2 + core, p)
        return pltpu.make_async_remote_copy(
            src_ref=other.at[at], dst_ref=other.at[at],
            send_sem=a_send.at[p], recv_sem=a_recv.at[p],
            device_id=a_peer, device_id_type=MESH,
        )

    def c_copy(p, late):
        at = piece_of((x_lo + late * (1 - 2 * x_lo)) * 2 + core, p)
        return pltpu.make_async_remote_copy(
            src_ref=other.at[at], dst_ref=other.at[at],
            send_sem=c_send.at[late, p], recv_sem=c_recv.at[late, p],
            device_id=c_peer, device_id_type=MESH,
        )

    def rows_of(i):
        return pl.ds(pl.multiple_of(i * chunk, chunk), chunk)

    def k_copy(i, which):
        return pltpu.make_async_remote_copy(
            src_ref=keys.at[which, rows_of(i)],
            dst_ref=out_ref.at[pl.ds(pl.multiple_of(served * half + i * chunk, chunk), chunk)],
            send_sem=k_send.at[which, i],
            recv_sem=k_recv.at[which, i],
            device_id=(a_peer, b_peer)[which],
            device_id_type=MESH,
        )

    raw_copy.wait()

    def arrange(i):
        def take(n, carry):
            e, xl, k = n // 4, (n // 2) % 2, n % 2
            to = ((z + shift_of(i, e)) % NZ) * PER_Z + xl * 2 + k
            first = raw[index_ref[to, 0]]
            second = raw[index_ref[to, 1]]
            away[i * 8 + n, 0] = first
            away[i * 8 + n, 1] = second

            @pl.when(self_step(i, n) > 0)
            def _():
                gath[0, i, x_hi, (e * 2 + x_lo) * 2] = first
                gath[0, i, x_hi, (e * 2 + x_lo) * 2 + 1] = second

            return carry

        lax.fori_loop(0, 8, take, 0)

    def send_all(i, carry):
        def send(n, inner):
            @pl.when(self_step(i, n) < 1)
            def _():
                z_copy(i, n).start()

            return inner

        lax.fori_loop(0, 8, send, 0)
        return carry

    def arrange_all(i, carry):
        arrange(i)
        return carry

    lax.fori_loop(0, CHUNKS, arrange_all, 0)
    pl.semaphore_wait(barrier, NZ * NX - keeps + 5)
    lax.fori_loop(0, CHUNKS, send_all, 0)

    for j in range(parts):
        weight_copy(j).wait()
    for p in range(PIECES):
        b_copy(p).start()
    for j in range(parts):
        gain_copy(j).wait()

    sub = 2 * BLK_ROWS

    def normalise(i):
        def norm_rows(n, carry):
            to = pl.ds(pl.multiple_of(i * chunk + n * sub, sub), sub)

            def values(j):
                held = gath[j // 2, i, j % 2, pl.ds(n * 2, 2)]
                return held.astype(jnp.float32).reshape(sub, depth)

            row_sum = 0.0
            row_sq = 0.0
            for j in range(parts):
                v = values(j)
                row_sum = row_sum + jnp.sum(v, axis=1, keepdims=True)
                row_sq = row_sq + jnp.sum(v * v, axis=1, keepdims=True)
            mean = row_sum / width
            scale = lax.rsqrt(row_sq / width - mean * mean + EPS)
            for j in range(parts):
                cols = pl.ds(j * depth, depth)
                normed[to, cols] = ((values(j) - mean) * scale * gains[:, cols]).astype(
                    jnp.bfloat16
                )
            return carry

        lax.fori_loop(0, chunk // sub, norm_rows, 0)

    def project(i, which):
        keys[which, rows_of(i), :] = jnp.dot(
            normed[rows_of(i), :], (weight, other)[which][...],
            preferred_element_type=jnp.float32,
        ).astype(jnp.bfloat16)
        k_copy(i, which).start()

    def step(k, carry):
        @pl.when(k < CHUNKS)
        def _():
            def arrived(m, inner):
                @pl.when(self_source(k, m) < 1)
                def _():
                    z_arrival(k, m).wait_recv()

                return inner

            lax.fori_loop(0, 8, arrived, 0)
            for way in range(2):
                y_copy(k, way).start()

        @pl.when((k > 0) & (k <= CHUNKS))
        def _():
            for way in range(2):
                y_copy(k - 1, way).wait_recv()
                f_copy(k - 1, way).start()

        @pl.when(k < PIECES // 2)
        def _():
            for p in range(2):
                b_copy(k * 2 + p).wait_recv()
                a_copy(k * 2 + p).start()
                c_copy(k * 2 + p, 0).start()

        @pl.when((k > 0) & (k <= PIECES // 2))
        def _():
            for p in range(2):
                a_copy(k * 2 - 2 + p).wait_send()
                pltpu.make_async_remote_copy(
                    src_ref=other.at[piece_of(x_lo * 2 + core, k * 2 - 2 + p)],
                    dst_ref=other.at[piece_of((1 - x_lo) * 2 + core, k * 2 - 2 + p)],
                    send_sem=a_send.at[k * 2 - 2 + p], recv_sem=a_recv.at[k * 2 - 2 + p],
                    device_id=a_peer, device_id_type=MESH,
                ).wait_recv()
                c_copy(k * 2 - 2 + p, 1).start()

        @pl.when(k > 1)
        def _():
            for way in range(2):
                f_copy(k - 2, way).wait_recv()
            normalise(k - 2)
            project(k - 2, 0)

        @pl.when(k == FIRST_OTHER)
        def _():
            for p in range(PIECES):
                for late in range(2):
                    side = x_lo + late * (1 - 2 * x_lo)
                    pltpu.make_async_remote_copy(
                        src_ref=other.at[piece_of(side * 2 + core, p)],
                        dst_ref=other.at[piece_of(side * 2 + 1 - core, p)],
                        send_sem=c_send.at[late, p], recv_sem=c_recv.at[late, p],
                        device_id=c_peer, device_id_type=MESH,
                    ).wait_recv()

        @pl.when(k >= FIRST_OTHER)
        def _():
            def one(i, inner):
                project(i, 1)
                return inner

            start = (k - 2) * jnp.minimum(k - FIRST_OTHER, 1)
            lax.fori_loop(start, k - 1, one, 0)

        return carry

    lax.fori_loop(0, CHUNKS + 2, step, 0)

    def z_sent(n, carry):
        @pl.when(self_step(n // 8, n % 8) < 1)
        def _():
            z_copy(n // 8, n % 8).wait_send()

        return carry

    lax.fori_loop(0, CHUNKS * 8, z_sent, 0)

    def finish(i, carry):
        for way in range(2):
            y_copy(i, way).wait_send()
            f_copy(i, way).wait_send()
        for which in range(2):
            k_copy(i, which).wait_send()
            source = served + (1 - which) * (1 - 2 * served)
            pltpu.make_async_remote_copy(
                src_ref=keys.at[which, rows_of(i)],
                dst_ref=out_ref.at[pl.ds(pl.multiple_of(source * half + i * chunk, chunk), chunk)],
                send_sem=k_send.at[which, i], recv_sem=k_recv.at[which, i],
                device_id=(a_peer, b_peer)[which], device_id_type=MESH,
            ).wait_recv()
        return carry

    lax.fori_loop(0, CHUNKS, finish, 0)
    for p in range(PIECES):
        b_copy(p).wait_send()
        for late in range(2):
            c_copy(p, late).wait_send()


def on_device(groups, parts, memory_rows, norm_gain, key_weight, owner_table):
    row_count, depth = memory_rows.shape
    columns = key_weight.shape[1]
    blocks = row_count // BLK_ROWS
    any_space = pl.BlockSpec(memory_space=pl.ANY)
    in_hbm = pl.BlockSpec(memory_space=pltpu.HBM)
    in_vmem = pl.BlockSpec(memory_space=pltpu.VMEM)
    in_smem = pl.BlockSpec(memory_space=pltpu.SMEM)

    dma = pltpu.SemaphoreType.DMA
    listing = jax.ShapeDtypeStruct((groups, blocks), jnp.int32)
    slots, index = pl.pallas_call(
        functools.partial(index_kernel, groups),
        out_shape=[listing, listing],
        in_specs=[in_vmem],
        out_specs=[in_vmem, in_vmem],
        compiler_params=pltpu.CompilerParams(vmem_limit_bytes=4 * MIB),
        name="index",
    )(owner_table.reshape(groups, blocks))

    chunk_blocks = blocks // 2 // CHUNKS
    incoming = pl.pallas_call(
        main_kernel,
        out_shape=jax.ShapeDtypeStruct((row_count, columns), jnp.bfloat16),
        in_specs=[in_smem, in_hbm, in_hbm, in_hbm],
        out_specs=any_space,
        scratch_shapes=[
            pltpu.VMEM((blocks, BLK_ROWS, depth), jnp.bfloat16),
            pltpu.VMEM((blocks // 2, 2, BLK_ROWS, depth), jnp.bfloat16),
            pltpu.VMEM((NY, CHUNKS, 2, chunk_blocks, BLK_ROWS, depth), jnp.bfloat16),
            pltpu.VMEM((depth * parts, columns), jnp.bfloat16),
            pltpu.VMEM((depth * parts, columns), jnp.bfloat16),
            pltpu.VMEM((2, row_count // 2, columns), jnp.bfloat16),
            pltpu.VMEM((row_count // 2, depth * parts), jnp.bfloat16),
            pltpu.VMEM((1, depth * parts), jnp.float32),
            dma,
            dma((parts,)),
            dma((parts,)),
            dma((CHUNKS * 8,)),
            dma((CHUNKS * 8,)),
            dma((2, CHUNKS)),
            dma((2, CHUNKS)),
            dma((2, CHUNKS)),
            dma((2, CHUNKS)),
            dma((PIECES,)),
            dma((PIECES,)),
            dma((PIECES,)),
            dma((PIECES,)),
            dma((2, PIECES)),
            dma((2, PIECES)),
            dma((2, CHUNKS)),
            dma((2, CHUNKS)),
        ],
        compiler_params=pltpu.CompilerParams(
            collective_id=0, has_side_effects=True, vmem_limit_bytes=48 * MIB
        ),
        name="exchange",
    )(index, memory_rows.reshape(blocks, BLK_ROWS, depth), norm_gain[None, :], key_weight)

    placed = pl.pallas_call(
        place_kernel,
        out_shape=jax.ShapeDtypeStruct((blocks, BLK_ROWS, columns), jnp.bfloat16),
        in_specs=[in_smem, in_vmem],
        out_specs=any_space,
        scratch_shapes=[pltpu.SemaphoreType.DMA],
        compiler_params=pltpu.CompilerParams(vmem_limit_bytes=16 * MIB),
        name="place",
    )(slots, incoming.reshape(blocks, BLK_ROWS, columns))
    return placed.reshape(row_count, columns)


def solution(mesh):
    in_specs = (P("grp", "tp"), P(), P(None, "tp"), P())
    out_specs = P("grp", "tp")
    return jax.shard_map(
        functools.partial(on_device, mesh.shape["grp"], mesh.shape["tp"]),
        mesh=mesh, in_specs=in_specs, out_specs=out_specs, check_vma=False,
    )
```

```python
import functools

import jax
import jax.numpy as jnp
from jax import lax
from jax.experimental import pallas as pl
from jax.experimental.pallas import tpu as pltpu
from jax.sharding import PartitionSpec as P

BLK_ROWS = 8
EPS = 1e-05
MIB = 1024 * 1024
MESH = pl.DeviceIdType.MESH

NZ = 16
NY = 4
NX = 4
PER_Z = 4
SHIFTS = (3, 13, 4, 12, 5, 11, 1, 15, 7, 9, 2, 14, 6, 10, 8, 0)
STEPS = len(SHIFTS)
HOME_STEPS = 6
PIECES = 8
OTHER_CHUNK = 7
FIRST_HAND = (0, 0, 2, 3, 5, 6, 8, 10)
SECOND_HAND = (2, 2, 4, 5, 7, 8, 10, 12)
AHEAD = 2


def wrapped(v, n):
    return jnp.where(v >= n, v - n, v)


def core_served(x):
    return ((x + 1) // 2 + 1) % 2


def index_kernel(groups, table_ref, slot_ref, index_ref):
    me = lax.axis_index("grp")
    blocks = table_ref.shape[1]
    capacity = blocks // groups
    lane = lax.broadcasted_iota(jnp.int32, (groups, blocks), 1)
    row = lax.broadcasted_iota(jnp.int32, (groups, blocks), 0)

    def ranked(offset, value):
        chosen = (offset >= 0) & (offset < blocks)
        counted = chosen.astype(jnp.int32)
        shift = 1
        while shift < blocks:
            counted = counted + jnp.where(lane >= shift, pltpu.roll(counted, shift, 1), 0)
            shift *= 2
        result = jnp.zeros((groups, blocks), jnp.int32)
        for r in range(capacity):
            at_rank = jnp.where(chosen & (counted == r + 1), value, 0).astype(jnp.float32)
            found = jnp.sum(at_rank, axis=1, keepdims=True).astype(jnp.int32)
            result = jnp.where(lane == r, found, result)
        return result

    own = jnp.broadcast_to(table_ref[pl.ds(me, 1), :], (groups, blocks))
    index_ref[...] = ranked(own - row * blocks, lane)
    offset = table_ref[...] - me * blocks
    slot_ref[...] = ranked(offset, offset)


def place_kernel(slot_ref, in_ref, out_ref, sem):
    z = lax.axis_index("grp") // PER_Z
    for s in range(2):
        for j in range(STEPS):
            first = wrapped(z + (NZ - SHIFTS[j]) % NZ, NZ) * PER_Z + s
            for a in range(2):
                for r in range(2):
                    n = ((s * STEPS + j) * 2 + a) * 2 + r
                    slot = slot_ref[first + a * 2, r]
                    pltpu.make_async_copy(in_ref.at[n], out_ref.at[slot], sem).start()
    pltpu.make_async_copy(in_ref, out_ref, sem).wait()


def main_kernel(
    index_ref, rows_ref, gain_ref, weight_ref, out_ref,
    away, gath, weight, other, keys, normed, gains,
    weight_sem, s_send, s_recv, z_send, z_recv, y_send, y_recv, f_send, f_recv,
    b_send, b_recv, a_send, a_recv, c_send, c_recv, k_send, k_recv, h_send, h_recv,
):
    g = lax.axis_index("grp")
    t = lax.axis_index("tp")
    z = g // PER_Z
    x_lo = (g // 2) % 2
    core = g % 2
    x_hi = t // NY
    y = t % NY
    x = x_lo + 2 * x_hi
    served = core_served(x)
    keeps = 1 - (served + core) % 2
    depth = rows_ref.shape[2]
    width = weight_ref.shape[0]
    parts = width // depth
    sub = 2 * BLK_ROWS
    chunk = 4 * sub
    half = 2 * STEPS * sub
    chunks = half // chunk
    home_chunks = HOME_STEPS // 2
    quarter = width // 4
    piece = quarter // PIECES

    def at_device(z_at, x_at, core_at):
        high = jnp.where(x_at >= 2, 1, 0)
        return {"grp": z_at * PER_Z + (x_at - 2 * high) * 2 + core_at, "tp": high * NY + y}

    a_peer = at_device(z, x + 1 - 2 * x_lo, core)
    b_peer = at_device(z, NX - 1 - x, core)
    c_peer = at_device(z, x, 1 - core)
    y_up, y_down = wrapped(y + 1, NY), wrapped(y + NY - 1, NY)
    up = {"grp": g, "tp": x_hi * NY + y_up}
    down = {"grp": g, "tp": x_hi * NY + y_down}

    barrier = pltpu.get_barrier_semaphore()

    def signal(peer):
        pl.semaphore_signal(barrier, inc=1, device_id=peer, device_id_type=MESH)

    for peer in (a_peer, b_peer, c_peer, up, down):
        signal(peer)

    for j in range(HOME_STEPS, STEPS):
        zs = wrapped(z + (NZ - SHIFTS[j]) % NZ, NZ)
        for m in range(NX):
            if SHIFTS[j] == 0 and m == 0:
                @pl.when(keeps < 1)
                def _():
                    signal(at_device(zs, x, served))
            else:
                signal(at_device(zs, wrapped(x + m, NX), served))
    for j in range(HOME_STEPS):
        zs = wrapped(z + (NZ - SHIFTS[j]) % NZ, NZ)
        for m in range(4):
            signal(at_device(zs, wrapped(2 * core + 1 + m % 2, NX), m // 2))

    def origin(j):
        r, h = j // 2, j % 2
        return h * NY + (y, y_down, y_up, wrapped(y + 2, NY))[r]

    def weight_copy(j):
        return pltpu.make_async_copy(
            weight_ref.at[pl.ds(pl.multiple_of(origin(j) * depth, depth), depth)],
            weight.at[pl.ds(j * depth, depth)],
            weight_sem.at[j],
        )

    for j in range(parts):
        weight_copy(j).start()
    for j in range(parts):
        gains[:, pl.ds(j * depth, depth)] = gain_ref[
            :, pl.ds(pl.multiple_of(origin(j) * depth, depth), depth)
        ]

    mine = [
        keeps * jnp.where((x_hi == m // 2) & (x_lo == m % 2), 1, 0) for m in range(4)
    ]
    stays = [
        keeps * jnp.where((core == n // 2) & (x_lo == 1 - n % 2), 1, 0) for n in range(4)
    ]
    last = STEPS - 1

    def s_copy(j, which):
        k = which * served + (1 - which) * (1 - served)
        return pltpu.make_async_remote_copy(
            src_ref=away.at[pl.ds(j * 4 + k * 2, 2)],
            dst_ref=gath.at[0, j, x_hi],
            send_sem=s_send.at[which, j],
            recv_sem=s_recv.at[which, j],
            device_id=(a_peer, b_peer)[which],
            device_id_type=MESH,
        )

    def s_arrival(j, which):
        return pltpu.make_async_remote_copy(
            src_ref=away.at[pl.ds(j * 4, 2)],
            dst_ref=gath.at[0, j, x_hi + which * (1 - 2 * x_hi)],
            send_sem=s_send.at[which, j],
            recv_sem=s_recv.at[which, j],
            device_id=(a_peer, b_peer)[which],
            device_id_type=MESH,
        )

    def z_copy(j, n):
        return pltpu.make_async_remote_copy(
            src_ref=away.at[j * 4 + n],
            dst_ref=gath.at[0, j, x_hi, x_lo],
            send_sem=z_send.at[j * 4 + n],
            recv_sem=z_recv.at[j * 4 + x_hi * 2 + x_lo],
            device_id=at_device(
                wrapped(z + SHIFTS[j], NZ), wrapped(2 * core + n % 2 + 1, NX), n // 2
            ),
            device_id_type=MESH,
        )

    def z_arrival(j, m):
        return pltpu.make_async_remote_copy(
            src_ref=away.at[j * 4 + m],
            dst_ref=gath.at[0, j, m // 2, m % 2],
            send_sem=z_send.at[j * 4 + m],
            recv_sem=z_recv.at[j * 4 + m],
            device_id=a_peer,
            device_id_type=MESH,
        )

    def y_copy(j, way):
        return pltpu.make_async_remote_copy(
            src_ref=gath.at[0, j],
            dst_ref=gath.at[1 + way, j],
            send_sem=y_send.at[way, j],
            recv_sem=y_recv.at[way, j],
            device_id=(up, down)[way],
            device_id_type=MESH,
        )

    def f_copy(j, way):
        return pltpu.make_async_remote_copy(
            src_ref=gath.at[1 + way, j, way],
            dst_ref=gath.at[3, j, way],
            send_sem=f_send.at[way, j],
            recv_sem=f_recv.at[way, j],
            device_id=(up, down)[way],
            device_id_type=MESH,
        )

    def piece_of(q, p):
        return pl.ds(pl.multiple_of(q * quarter + p * piece, piece), piece)

    def b_copy(p):
        at = piece_of((1 - x_lo) * 2 + core, p)
        return pltpu.make_async_remote_copy(
            src_ref=weight.at[at], dst_ref=other.at[at],
            send_sem=b_send.at[p], recv_sem=b_recv.at[p],
            device_id=b_peer, device_id_type=MESH,
        )

    def b_arrival(p):
        at = piece_of(x_lo * 2 + core, p)
        return pltpu.make_async_remote_copy(
            src_ref=weight.at[at], dst_ref=other.at[at],
            send_sem=b_send.at[p], recv_sem=b_recv.at[p],
            device_id=b_peer, device_id_type=MESH,
        )

    def a_copy(p, side):
        at = piece_of((x_lo + side * (1 - 2 * x_lo)) * 2 + core, p)
        return pltpu.make_async_remote_copy(
            src_ref=other.at[at], dst_ref=other.at[at],
            send_sem=a_send.at[p], recv_sem=a_recv.at[p],
            device_id=a_peer, device_id_type=MESH,
        )

    def c_copy(p, late, at_core):
        at = piece_of((x_lo + late * (1 - 2 * x_lo)) * 2 + at_core, p)
        return pltpu.make_async_remote_copy(
            src_ref=other.at[at], dst_ref=other.at[at],
            send_sem=c_send.at[late, p], recv_sem=c_recv.at[late, p],
            device_id=c_peer, device_id_type=MESH,
        )

    def rows_of(i):
        return pl.ds(pl.multiple_of(i * chunk, chunk), chunk)

    def k_copy(i, which, source):
        return pltpu.make_async_remote_copy(
            src_ref=keys.at[which, rows_of(i)],
            dst_ref=out_ref.at[pl.ds(pl.multiple_of(source * half + i * chunk, chunk), chunk)],
            send_sem=k_send.at[which, i],
            recv_sem=k_recv.at[which, i],
            device_id=(a_peer, b_peer)[which],
            device_id_type=MESH,
        )

    def h_copy(n, which):
        side = x_hi + which * (1 - 2 * x_hi)
        at = (core * STEPS + n // 2) * 2 + 1 - x_lo
        return pltpu.make_async_remote_copy(
            src_ref=keys.at[which, pl.ds(pl.multiple_of(n * sub, sub), sub)],
            dst_ref=out_ref.at[pl.ds(pl.multiple_of(at * sub, sub), sub)],
            send_sem=h_send.at[which, n],
            recv_sem=h_recv.at[core, n // 2 * 2 + 1 - x_lo],
            device_id=at_device(wrapped(z + SHIFTS[n // 2], NZ), n % 2 + 2 * side, served),
            device_id_type=MESH,
        )

    def h_arrival(n, s):
        return pltpu.make_async_remote_copy(
            src_ref=keys.at[0, pl.ds(pl.multiple_of(n * sub, sub), sub)],
            dst_ref=out_ref.at[pl.ds(pl.multiple_of((s * STEPS * 2 + n) * sub, sub), sub)],
            send_sem=h_send.at[0, n],
            recv_sem=h_recv.at[s, n],
            device_id=a_peer,
            device_id_type=MESH,
        )

    def arrange(j):
        to_z = wrapped(z + SHIFTS[j], NZ) * PER_Z
        for n in range(4):
            to = to_z + (n % 2) * 2 + n // 2
            first = rows_ref[index_ref[to, 0]]
            second = rows_ref[index_ref[to, 1]]
            away[j * 4 + n, 0] = first
            away[j * 4 + n, 1] = second
            if j == last:
                @pl.when(stays[n] > 0)
                def _():
                    gath[0, j, x_hi, x_lo, 0] = first
                    gath[0, j, x_hi, x_lo, 1] = second

    for j in range(STEPS):
        arrange(j)
    pl.semaphore_wait(barrier, STEPS * 4 - keeps + 5)
    for j in range(HOME_STEPS):
        for which in range(2):
            s_copy(j, which).start()
    for j in range(HOME_STEPS, STEPS):
        for n in range(4):
            if j == last:
                @pl.when(stays[n] < 1)
                def _():
                    z_copy(j, n).start()
            else:
                z_copy(j, n).start()

    for j in range(parts):
        weight_copy(j).wait()
    for p in range(PIECES):
        b_copy(p).start()

    def normalise(i):
        def norm_rows(n, carry):
            to = pl.ds(pl.multiple_of(i * chunk + n * sub, sub), sub)

            def values(j):
                held = gath[j // 2, i * 2 + n // 2, j % 2, n - n // 2 * 2]
                return held.astype(jnp.float32).reshape(sub, depth)

            row_sum = 0.0
            row_sq = 0.0
            for j in range(parts):
                v = values(j)
                row_sum = row_sum + jnp.sum(v, axis=1, keepdims=True)
                row_sq = row_sq + jnp.sum(v * v, axis=1, keepdims=True)
            mean = row_sum / width
            scale = lax.rsqrt(row_sq / width - mean * mean + EPS)
            for j in range(parts):
                cols = pl.ds(j * depth, depth)
                normed[to, cols] = ((values(j) - mean) * scale * gains[:, cols]).astype(
                    jnp.bfloat16
                )
            return carry

        lax.fori_loop(0, chunk // sub, norm_rows, 0)

    def project(start, count, which):
        at = pl.ds(pl.multiple_of(start, chunk), count)
        keys[which, at, :] = jnp.dot(
            normed[at, :], (weight, other)[which][...], preferred_element_type=jnp.float32
        ).astype(jnp.bfloat16)

    def rows_arrived(i, e):
        for m in range(4):
            if e == last % 2:
                @pl.when((i < chunks - 1) | (mine[m] < 1))
                def _():
                    z_arrival(i * 2 + e, m).wait_recv()
            else:
                z_arrival(i * 2 + e, m).wait_recv()

    def forward(j):
        for way in range(2):
            y_copy(j, way).wait_recv()
            f_copy(j, way).start()

    def start_ring(j):
        for way in range(2):
            y_copy(j, way).start()

    def step(i, carry):
        for e in range(2):
            @pl.when(i < chunks)
            def _():
                forward(i * 2 + e)

            @pl.when((i + AHEAD >= home_chunks) & (i + AHEAD < chunks))
            def _():
                rows_arrived(i + AHEAD, e)
                start_ring((i + AHEAD) * 2 + e)

            for p in range(PIECES):
                if FIRST_HAND[p] % 2 == e:
                    @pl.when(i == FIRST_HAND[p] // 2)
                    def _():
                        b_arrival(p).wait_recv()
                        a_copy(p, 0).start()
                        c_copy(p, 0, core).start()

            for p in range(PIECES):
                if SECOND_HAND[p] % 2 == e:
                    @pl.when(i == SECOND_HAND[p] // 2)
                    def _():
                        a_copy(p, 1).wait_recv()
                        c_copy(p, 1, core).start()

        @pl.when(i > 0)
        def _():
            c = i - 1
            for e in range(2):
                for way in range(2):
                    f_copy(c * 2 + e, way).wait_recv()
            normalise(c)
            project(c * chunk, chunk, 0)

            for home in range(home_chunks):
                @pl.when(c == home)
                def _():
                    for n in range(home * 4, home * 4 + 4):
                        h_copy(n, 0).start()

            @pl.when(c >= home_chunks)
            def _():
                k_copy(c, 0, served).start()

        @pl.when(i == OTHER_CHUNK)
        def _():
            for p in range(PIECES):
                for late in range(2):
                    c_copy(p, late, 1 - core).wait_recv()
            project(0, home_chunks * chunk, 1)
            for n in range(home_chunks * 4):
                h_copy(n, 1).start()
            project(home_chunks * chunk, (OTHER_CHUNK - home_chunks) * chunk, 1)
            for c in range(home_chunks, OTHER_CHUNK):
                k_copy(c, 1, served).start()

        @pl.when(i > OTHER_CHUNK)
        def _():
            project((i - 1) * chunk, chunk, 1)
            k_copy(i - 1, 1, served).start()

        return carry

    for j in range(HOME_STEPS):
        for which in range(2):
            s_arrival(j, which).wait_recv()
        start_ring(j)
    lax.fori_loop(0, chunks + 1, step, 0)

    for j in range(HOME_STEPS, STEPS):
        for n in range(4):
            if j == last:
                @pl.when(stays[n] < 1)
                def _():
                    z_copy(j, n).wait_send()
            else:
                z_copy(j, n).wait_send()

    def home_sent(j, carry):
        for which in range(2):
            s_copy(j, which).wait_send()
        return carry

    def ring_sent(j, carry):
        for way in range(2):
            y_copy(j, way).wait_send()
            f_copy(j, way).wait_send()
        return carry

    def weight_sent(p, carry):
        b_copy(p).wait_send()
        a_copy(p, 0).wait_send()
        for late in range(2):
            c_copy(p, late, core).wait_send()
        return carry

    def keys_done(i, carry):
        for which in range(2):
            k_copy(i, which, served).wait_send()
            k_copy(i, which, served + (1 - which) * (1 - 2 * served)).wait_recv()
        return carry

    for n in range(HOME_STEPS * 2):
        for which in range(2):
            h_copy(n, which).wait_send()
            h_arrival(n, which).wait_recv()
    lax.fori_loop(0, HOME_STEPS, home_sent, 0)
    lax.fori_loop(0, STEPS, ring_sent, 0)
    lax.fori_loop(0, PIECES, weight_sent, 0)
    lax.fori_loop(home_chunks, chunks, keys_done, 0)


def on_device(groups, parts, memory_rows, norm_gain, key_weight, owner_table):
    row_count, depth = memory_rows.shape
    columns = key_weight.shape[1]
    blocks = row_count // BLK_ROWS
    any_space = pl.BlockSpec(memory_space=pl.ANY)
    in_hbm = pl.BlockSpec(memory_space=pltpu.HBM)
    in_vmem = pl.BlockSpec(memory_space=pltpu.VMEM)
    in_smem = pl.BlockSpec(memory_space=pltpu.SMEM)

    dma = pltpu.SemaphoreType.DMA
    listing = jax.ShapeDtypeStruct((groups, blocks), jnp.int32)
    slots, index = pl.pallas_call(
        functools.partial(index_kernel, groups),
        out_shape=[listing, listing],
        in_specs=[in_vmem],
        out_specs=[in_vmem, in_vmem],
        compiler_params=pltpu.CompilerParams(vmem_limit_bytes=4 * MIB),
        name="index",
    )(owner_table.reshape(groups, blocks))

    chunks = blocks // 16
    incoming = pl.pallas_call(
        main_kernel,
        out_shape=jax.ShapeDtypeStruct((row_count, columns), jnp.bfloat16),
        in_specs=[in_smem, in_vmem, in_vmem, in_hbm],
        out_specs=any_space,
        scratch_shapes=[
            pltpu.VMEM((STEPS * 4, 2, BLK_ROWS, depth), jnp.bfloat16),
            pltpu.VMEM((NY, STEPS, 2, 2, 2, BLK_ROWS, depth), jnp.bfloat16),
            pltpu.VMEM((depth * parts, columns), jnp.bfloat16),
            pltpu.VMEM((depth * parts, columns), jnp.bfloat16),
            pltpu.VMEM((2, row_count // 2, columns), jnp.bfloat16),
            pltpu.VMEM((row_count // 2, depth * parts), jnp.bfloat16),
            pltpu.VMEM((1, depth * parts), jnp.float32),
            dma((parts,)),
            dma((2, HOME_STEPS)),
            dma((2, HOME_STEPS)),
            dma((STEPS * 4,)),
            dma((STEPS * 4,)),
            dma((2, STEPS)),
            dma((2, STEPS)),
            dma((2, STEPS)),
            dma((2, STEPS)),
            dma((PIECES,)),
            dma((PIECES,)),
            dma((PIECES,)),
            dma((PIECES,)),
            dma((2, PIECES)),
            dma((2, PIECES)),
            dma((2, chunks)),
            dma((2, chunks)),
            dma((2, HOME_STEPS * 2)),
            dma((2, HOME_STEPS * 2)),
        ],
        compiler_params=pltpu.CompilerParams(
            collective_id=0, has_side_effects=True, vmem_limit_bytes=48 * MIB
        ),
        name="exchange",
    )(index, memory_rows.reshape(blocks, BLK_ROWS, depth), norm_gain[None, :], key_weight)

    placed = pl.pallas_call(
        place_kernel,
        out_shape=jax.ShapeDtypeStruct((blocks, BLK_ROWS, columns), jnp.bfloat16),
        in_specs=[in_smem, in_vmem],
        out_specs=any_space,
        scratch_shapes=[pltpu.SemaphoreType.DMA],
        compiler_params=pltpu.CompilerParams(vmem_limit_bytes=16 * MIB),
        name="place",
    )(slots, incoming.reshape(blocks, BLK_ROWS, columns))
    return placed.reshape(row_count, columns)


def solution(mesh):
    in_specs = (P("grp", "tp"), P(), P(None, "tp"), P())
    out_specs = P("grp", "tp")
    return jax.shard_map(
        functools.partial(on_device, mesh.shape["grp"], mesh.shape["tp"]),
        mesh=mesh, in_specs=in_specs, out_specs=out_specs, check_vma=False,
    )
```

```python
import functools

import jax
import jax.numpy as jnp
from jax import lax
from jax.experimental import pallas as pl
from jax.experimental.pallas import tpu as pltpu
from jax.sharding import PartitionSpec as P

BLK_ROWS = 8
EPS = 1e-05
MIB = 1024 * 1024
MESH = pl.DeviceIdType.MESH

NZ = 16
NY = 4
NX = 4
PER_Z = 4
SHIFTS = (3, 13, 4, 12, 5, 11, 1, 15, 2, 14, 6, 10, 7, 9, 8, 0)
STEPS = len(SHIFTS)
HOME_STEPS = 6
PIECES = 8
OTHER_CHUNK = 7
FIRST_HAND = (1, 2, 3, 4, 6, 7, 8, 9)
SECOND_HAND = (3, 4, 5, 6, 8, 9, 10, 12)
AHEAD = 2


def wrapped(v, n):
    return jnp.where(v >= n, v - n, v)


def core_served(x):
    return ((x + 1) // 2 + 1) % 2


def index_kernel(groups, table_ref, slot_ref, index_ref):
    me = lax.axis_index("grp")
    blocks = table_ref.shape[1]
    capacity = blocks // groups
    lane = lax.broadcasted_iota(jnp.int32, (groups, blocks), 1)
    row = lax.broadcasted_iota(jnp.int32, (groups, blocks), 0)

    def ranked(offset, value):
        chosen = (offset >= 0) & (offset < blocks)
        counted = chosen.astype(jnp.int32)
        shift = 1
        while shift < blocks:
            counted = counted + jnp.where(lane >= shift, pltpu.roll(counted, shift, 1), 0)
            shift *= 2
        result = jnp.zeros((groups, blocks), jnp.int32)
        for r in range(capacity):
            at_rank = jnp.where(chosen & (counted == r + 1), value, 0).astype(jnp.float32)
            found = jnp.sum(at_rank, axis=1, keepdims=True).astype(jnp.int32)
            result = jnp.where(lane == r, found, result)
        return result

    own = jnp.broadcast_to(table_ref[pl.ds(me, 1), :], (groups, blocks))
    index_ref[...] = ranked(own - row * blocks, lane)
    offset = table_ref[...] - me * blocks
    slot_ref[...] = ranked(offset, offset)


def place_kernel(slot_ref, in_ref, out_ref, sem):
    z = lax.axis_index("grp") // PER_Z
    for s in range(2):
        for j in range(STEPS):
            first = wrapped(z + (NZ - SHIFTS[j]) % NZ, NZ) * PER_Z + s
            for a in range(2):
                for r in range(2):
                    n = ((s * STEPS + j) * 2 + a) * 2 + r
                    slot = slot_ref[first + a * 2, r]
                    pltpu.make_async_copy(in_ref.at[n], out_ref.at[slot], sem).start()
    pltpu.make_async_copy(in_ref, out_ref, sem).wait()


def main_kernel(
    index_ref, rows_ref, gain_ref, weight_ref, out_ref,
    raw, away, gath, weight, other, keys, normed, gains,
    raw_sem, weight_sem, gain_sem, s_send, s_recv, z_send, z_recv, y_send, y_recv, f_send, f_recv,
    b_send, b_recv, a_send, a_recv, c_send, c_recv, k_send, k_recv, h_send, h_recv,
    token,
):
    g = lax.axis_index("grp")
    t = lax.axis_index("tp")
    z = g // PER_Z
    x_lo = (g // 2) % 2
    core = g % 2
    x_hi = t // NY
    y = t % NY
    x = x_lo + 2 * x_hi
    served = core_served(x)
    keeps = 1 - (served + core) % 2
    depth = rows_ref.shape[2]
    width = weight_ref.shape[0]
    parts = width // depth
    sub = 2 * BLK_ROWS
    chunk = 4 * sub
    half = 2 * STEPS * sub
    chunks = half // chunk
    home_chunks = HOME_STEPS // 2
    quarter = width // 4
    piece = quarter // PIECES

    def at_device(z_at, x_at, core_at):
        high = jnp.where(x_at >= 2, 1, 0)
        return {"grp": z_at * PER_Z + (x_at - 2 * high) * 2 + core_at, "tp": high * NY + y}

    a_peer = at_device(z, x + 1 - 2 * x_lo, core)
    b_peer = at_device(z, NX - 1 - x, core)
    c_peer = at_device(z, x, 1 - core)
    raw_copy = pltpu.make_async_copy(rows_ref, raw, raw_sem)
    raw_copy.start()

    y_up, y_down = wrapped(y + 1, NY), wrapped(y + NY - 1, NY)
    up = {"grp": g, "tp": x_hi * NY + y_up}
    down = {"grp": g, "tp": x_hi * NY + y_down}

    barrier = pltpu.get_barrier_semaphore()

    def signal(peer):
        pl.semaphore_signal(barrier, inc=1, device_id=peer, device_id_type=MESH)

    z_up = at_device(wrapped(z + 1, NZ), x, core)
    z_down = at_device(wrapped(z + NZ - 1, NZ), x, core)
    for peer in (up, down, z_up, z_down, c_peer):
        signal(peer)
    for m in range(1, NX):
        for k in range(2):
            signal(at_device(z, wrapped(x + m, NX), k))

    def origin(j):
        r, h = j // 2, j % 2
        return h * NY + (y, y_down, y_up, wrapped(y + 2, NY))[r]

    def weight_copy(j):
        return pltpu.make_async_copy(
            weight_ref.at[pl.ds(pl.multiple_of(origin(j) * depth, depth), depth)],
            weight.at[pl.ds(j * depth, depth)],
            weight_sem.at[j],
        )

    def gain_copy(j):
        return pltpu.make_async_copy(
            gain_ref.at[:, pl.ds(pl.multiple_of(origin(j) * depth, depth), depth)],
            gains.at[:, pl.ds(j * depth, depth)],
            gain_sem.at[j],
        )

    for j in range(parts):
        weight_copy(j).start()
    for j in range(parts):
        gain_copy(j).start()

    mine = [
        keeps * jnp.where((x_hi == m // 2) & (x_lo == m % 2), 1, 0) for m in range(4)
    ]
    stays = [
        keeps * jnp.where((core == n // 2) & (x_lo == 1 - n % 2), 1, 0) for n in range(4)
    ]
    last = STEPS - 1

    def s_copy(j, which):
        k = which * served + (1 - which) * (1 - served)
        return pltpu.make_async_remote_copy(
            src_ref=away.at[pl.ds(j * 4 + k * 2, 2)],
            dst_ref=gath.at[0, j, x_hi],
            send_sem=s_send.at[which, j],
            recv_sem=s_recv.at[which, j],
            device_id=(a_peer, b_peer)[which],
            device_id_type=MESH,
        )

    def s_arrival(j, which):
        return pltpu.make_async_remote_copy(
            src_ref=away.at[pl.ds(j * 4, 2)],
            dst_ref=gath.at[0, j, x_hi + which * (1 - 2 * x_hi)],
            send_sem=s_send.at[which, j],
            recv_sem=s_recv.at[which, j],
            device_id=(a_peer, b_peer)[which],
            device_id_type=MESH,
        )

    def z_copy(j, n):
        return pltpu.make_async_remote_copy(
            src_ref=away.at[j * 4 + n],
            dst_ref=gath.at[0, j, x_hi, x_lo],
            send_sem=z_send.at[j * 4 + n],
            recv_sem=z_recv.at[j * 4 + x_hi * 2 + x_lo],
            device_id=at_device(
                wrapped(z + SHIFTS[j], NZ), wrapped(2 * core + n % 2 + 1, NX), n // 2
            ),
            device_id_type=MESH,
        )

    def z_arrival(j, m):
        return pltpu.make_async_remote_copy(
            src_ref=away.at[j * 4 + m],
            dst_ref=gath.at[0, j, m // 2, m % 2],
            send_sem=z_send.at[j * 4 + m],
            recv_sem=z_recv.at[j * 4 + m],
            device_id=a_peer,
            device_id_type=MESH,
        )

    def y_copy(j, way):
        return pltpu.make_async_remote_copy(
            src_ref=gath.at[0, j],
            dst_ref=gath.at[1 + way, j],
            send_sem=y_send.at[way, j],
            recv_sem=y_recv.at[way, j],
            device_id=(up, down)[way],
            device_id_type=MESH,
        )

    def f_copy(j, way):
        return pltpu.make_async_remote_copy(
            src_ref=gath.at[1 + way, j, way],
            dst_ref=gath.at[3, j, way],
            send_sem=f_send.at[way, j],
            recv_sem=f_recv.at[way, j],
            device_id=(up, down)[way],
            device_id_type=MESH,
        )

    def piece_of(q, p):
        return pl.ds(pl.multiple_of(q * quarter + p * piece, piece), piece)

    def b_copy(p):
        at = piece_of((1 - x_lo) * 2 + core, p)
        return pltpu.make_async_remote_copy(
            src_ref=weight.at[at], dst_ref=other.at[at],
            send_sem=b_send.at[p], recv_sem=b_recv.at[p],
            device_id=b_peer, device_id_type=MESH,
        )

    def b_arrival(p):
        at = piece_of(x_lo * 2 + core, p)
        return pltpu.make_async_remote_copy(
            src_ref=weight.at[at], dst_ref=other.at[at],
            send_sem=b_send.at[p], recv_sem=b_recv.at[p],
            device_id=b_peer, device_id_type=MESH,
        )

    def a_copy(p, side):
        at = piece_of((x_lo + side * (1 - 2 * x_lo)) * 2 + core, p)
        return pltpu.make_async_remote_copy(
            src_ref=other.at[at], dst_ref=other.at[at],
            send_sem=a_send.at[p], recv_sem=a_recv.at[p],
            device_id=a_peer, device_id_type=MESH,
        )

    def c_copy(p, late, at_core):
        at = piece_of((x_lo + late * (1 - 2 * x_lo)) * 2 + at_core, p)
        return pltpu.make_async_remote_copy(
            src_ref=other.at[at], dst_ref=other.at[at],
            send_sem=c_send.at[late, p], recv_sem=c_recv.at[late, p],
            device_id=c_peer, device_id_type=MESH,
        )

    def rows_of(i):
        return pl.ds(pl.multiple_of(i * chunk, chunk), chunk)

    def k_copy(i, which, source):
        return pltpu.make_async_remote_copy(
            src_ref=keys.at[which, rows_of(i)],
            dst_ref=out_ref.at[pl.ds(pl.multiple_of(source * half + i * chunk, chunk), chunk)],
            send_sem=k_send.at[which, i],
            recv_sem=k_recv.at[which, i],
            device_id=(a_peer, b_peer)[which],
            device_id_type=MESH,
        )

    def h_copy(n, which):
        side = x_hi + which * (1 - 2 * x_hi)
        at = (core * STEPS + n // 2) * 2 + 1 - x_lo
        return pltpu.make_async_remote_copy(
            src_ref=keys.at[which, pl.ds(pl.multiple_of(n * sub, sub), sub)],
            dst_ref=out_ref.at[pl.ds(pl.multiple_of(at * sub, sub), sub)],
            send_sem=h_send.at[which, n],
            recv_sem=h_recv.at[core, n // 2 * 2 + 1 - x_lo],
            device_id=at_device(wrapped(z + SHIFTS[n // 2], NZ), n % 2 + 2 * side, served),
            device_id_type=MESH,
        )

    def h_arrival(n, s):
        return pltpu.make_async_remote_copy(
            src_ref=keys.at[0, pl.ds(pl.multiple_of(n * sub, sub), sub)],
            dst_ref=out_ref.at[pl.ds(pl.multiple_of((s * STEPS * 2 + n) * sub, sub), sub)],
            send_sem=h_send.at[0, n],
            recv_sem=h_recv.at[s, n],
            device_id=a_peer,
            device_id_type=MESH,
        )

    def arrange(j):
        to_z = wrapped(z + SHIFTS[j], NZ) * PER_Z
        for n in range(4):
            to = to_z + (n % 2) * 2 + n // 2
            first = raw[index_ref[to, 0]]
            second = raw[index_ref[to, 1]]
            away[j * 4 + n, 0] = first
            away[j * 4 + n, 1] = second
            if j == last:
                @pl.when(stays[n] > 0)
                def _():
                    gath[0, j, x_hi, x_lo, 0] = first
                    gath[0, j, x_hi, x_lo, 1] = second

    raw_copy.wait()
    for j in range(STEPS):
        arrange(j)
    pl.semaphore_wait(barrier, 5 + 2 * (NX - 1))
    for j in range(HOME_STEPS):
        for which in range(2):
            s_copy(j, which).start()

    def send_rows(shift):
        j = SHIFTS.index(shift)
        for n in range(4):
            if j == last:
                @pl.when(stays[n] < 1)
                def _():
                    z_copy(j, n).start()
            else:
                z_copy(j, n).start()

    def start_ring(j):
        for way in range(2):
            y_copy(j, way).start()

    def start_home(j):
        for which in range(2):
            s_arrival(j, which).wait_recv()
        start_ring(j)

    for d in range(1, NZ // 2 + 1):
        ways = 2 if d < NZ // 2 else 1
        for way in range(ways):
            pl.semaphore_signal(
                token.at[way, d - 1], inc=1, device_id=(z_up, z_down)[way], device_id_type=MESH
            )
        if d == 1:
            send_rows(0)
            for j in range(parts):
                weight_copy(j).wait()
            for p in range(PIECES):
                b_copy(p).start()
        for way in range(ways):
            pl.semaphore_wait(token.at[way, d - 1], 1)
        for shift in sorted({d, NZ - d}):
            if shift in SHIFTS[HOME_STEPS:]:
                send_rows(shift)
        if d == 5:
            start_home(0)
            start_home(1)
        if d == 7:
            start_home(2)
            start_home(3)
    for j in range(4, HOME_STEPS):
        start_home(j)
    for j in range(parts):
        gain_copy(j).wait()

    sub = 2 * BLK_ROWS

    def normalise(i):
        def norm_rows(n, carry):
            to = pl.ds(pl.multiple_of(i * chunk + n * sub, sub), sub)

            def values(j):
                held = gath[j // 2, i * 2 + n // 2, j % 2, n - n // 2 * 2]
                return held.astype(jnp.float32).reshape(sub, depth)

            row_sum = 0.0
            row_sq = 0.0
            for j in range(parts):
                v = values(j)
                row_sum = row_sum + jnp.sum(v, axis=1, keepdims=True)
                row_sq = row_sq + jnp.sum(v * v, axis=1, keepdims=True)
            mean = row_sum / width
            scale = lax.rsqrt(row_sq / width - mean * mean + EPS)
            for j in range(parts):
                cols = pl.ds(j * depth, depth)
                normed[to, cols] = ((values(j) - mean) * scale * gains[:, cols]).astype(
                    jnp.bfloat16
                )
            return carry

        lax.fori_loop(0, chunk // sub, norm_rows, 0)

    def project(start, count, which):
        at = pl.ds(pl.multiple_of(start, chunk), count)
        keys[which, at, :] = jnp.dot(
            normed[at, :], (weight, other)[which][...], preferred_element_type=jnp.float32
        ).astype(jnp.bfloat16)

    def rows_arrived(i, e):
        for m in range(4):
            if e == last % 2:
                @pl.when((i < chunks - 1) | (mine[m] < 1))
                def _():
                    z_arrival(i * 2 + e, m).wait_recv()
            else:
                z_arrival(i * 2 + e, m).wait_recv()

    def forward(j):
        for way in range(2):
            y_copy(j, way).wait_recv()
            f_copy(j, way).start()

    def step(i, carry):
        for e in range(2):
            @pl.when(i < chunks)
            def _():
                forward(i * 2 + e)

            @pl.when((i + AHEAD >= home_chunks) & (i + AHEAD < chunks))
            def _():
                rows_arrived(i + AHEAD, e)
                start_ring((i + AHEAD) * 2 + e)

            for p in range(PIECES):
                if FIRST_HAND[p] % 2 == e:
                    @pl.when(i == FIRST_HAND[p] // 2)
                    def _():
                        b_arrival(p).wait_recv()
                        a_copy(p, 0).start()
                        c_copy(p, 0, core).start()

            for p in range(PIECES):
                if SECOND_HAND[p] % 2 == e:
                    @pl.when(i == SECOND_HAND[p] // 2)
                    def _():
                        a_copy(p, 1).wait_recv()
                        c_copy(p, 1, core).start()

        @pl.when(i > 0)
        def _():
            c = i - 1
            for e in range(2):
                for way in range(2):
                    f_copy(c * 2 + e, way).wait_recv()
            normalise(c)
            project(c * chunk, chunk, 0)

            for home in range(home_chunks):
                @pl.when(c == home)
                def _():
                    for n in range(home * 4, home * 4 + 4):
                        h_copy(n, 0).start()

            @pl.when(c >= home_chunks)
            def _():
                k_copy(c, 0, served).start()

        @pl.when(i == OTHER_CHUNK)
        def _():
            for p in range(PIECES):
                for late in range(2):
                    c_copy(p, late, 1 - core).wait_recv()
            project(0, home_chunks * chunk, 1)
            for n in range(home_chunks * 4):
                h_copy(n, 1).start()
            project(home_chunks * chunk, (OTHER_CHUNK - home_chunks) * chunk, 1)
            for c in range(home_chunks, OTHER_CHUNK):
                k_copy(c, 1, served).start()

        @pl.when(i > OTHER_CHUNK)
        def _():
            project((i - 1) * chunk, chunk, 1)
            k_copy(i - 1, 1, served).start()

        return carry

    lax.fori_loop(0, chunks + 1, step, 0)

    for j in range(HOME_STEPS, STEPS):
        for n in range(4):
            if j == last:
                @pl.when(stays[n] < 1)
                def _():
                    z_copy(j, n).wait_send()
            else:
                z_copy(j, n).wait_send()

    def home_sent(j, carry):
        for which in range(2):
            s_copy(j, which).wait_send()
        return carry

    def ring_sent(j, carry):
        for way in range(2):
            y_copy(j, way).wait_send()
            f_copy(j, way).wait_send()
        return carry

    def weight_sent(p, carry):
        b_copy(p).wait_send()
        a_copy(p, 0).wait_send()
        for late in range(2):
            c_copy(p, late, core).wait_send()
        return carry

    def keys_done(i, carry):
        for which in range(2):
            k_copy(i, which, served).wait_send()
            k_copy(i, which, served + (1 - which) * (1 - 2 * served)).wait_recv()
        return carry

    for n in range(HOME_STEPS * 2):
        for which in range(2):
            h_copy(n, which).wait_send()
            h_arrival(n, which).wait_recv()
    lax.fori_loop(0, HOME_STEPS, home_sent, 0)
    lax.fori_loop(0, STEPS, ring_sent, 0)
    lax.fori_loop(0, PIECES, weight_sent, 0)
    lax.fori_loop(home_chunks, chunks, keys_done, 0)


def on_device(groups, parts, memory_rows, norm_gain, key_weight, owner_table):
    row_count, depth = memory_rows.shape
    columns = key_weight.shape[1]
    blocks = row_count // BLK_ROWS
    any_space = pl.BlockSpec(memory_space=pl.ANY)
    in_hbm = pl.BlockSpec(memory_space=pltpu.HBM)
    in_vmem = pl.BlockSpec(memory_space=pltpu.VMEM)
    in_smem = pl.BlockSpec(memory_space=pltpu.SMEM)

    dma = pltpu.SemaphoreType.DMA
    listing = jax.ShapeDtypeStruct((groups, blocks), jnp.int32)
    slots, index = pl.pallas_call(
        functools.partial(index_kernel, groups),
        out_shape=[listing, listing],
        in_specs=[in_vmem],
        out_specs=[in_vmem, in_vmem],
        compiler_params=pltpu.CompilerParams(vmem_limit_bytes=4 * MIB),
        name="index",
    )(owner_table.reshape(groups, blocks))

    chunks = blocks // 16
    incoming = pl.pallas_call(
        main_kernel,
        out_shape=jax.ShapeDtypeStruct((row_count, columns), jnp.bfloat16),
        in_specs=[in_smem, in_hbm, in_hbm, in_hbm],
        out_specs=any_space,
        scratch_shapes=[
            pltpu.VMEM((blocks, BLK_ROWS, depth), jnp.bfloat16),
            pltpu.VMEM((STEPS * 4, 2, BLK_ROWS, depth), jnp.bfloat16),
            pltpu.VMEM((NY, STEPS, 2, 2, 2, BLK_ROWS, depth), jnp.bfloat16),
            pltpu.VMEM((depth * parts, columns), jnp.bfloat16),
            pltpu.VMEM((depth * parts, columns), jnp.bfloat16),
            pltpu.VMEM((2, row_count // 2, columns), jnp.bfloat16),
            pltpu.VMEM((row_count // 2, depth * parts), jnp.bfloat16),
            pltpu.VMEM((1, depth * parts), jnp.float32),
            dma,
            dma((parts,)),
            dma((parts,)),
            dma((2, HOME_STEPS)),
            dma((2, HOME_STEPS)),
            dma((STEPS * 4,)),
            dma((STEPS * 4,)),
            dma((2, STEPS)),
            dma((2, STEPS)),
            dma((2, STEPS)),
            dma((2, STEPS)),
            dma((PIECES,)),
            dma((PIECES,)),
            dma((PIECES,)),
            dma((PIECES,)),
            dma((2, PIECES)),
            dma((2, PIECES)),
            dma((2, chunks)),
            dma((2, chunks)),
            dma((2, HOME_STEPS * 2)),
            dma((2, HOME_STEPS * 2)),
            pltpu.SemaphoreType.REGULAR((2, NZ // 2)),
        ],
        compiler_params=pltpu.CompilerParams(
            collective_id=0, has_side_effects=True, vmem_limit_bytes=52 * MIB
        ),
        name="exchange",
    )(index, memory_rows.reshape(blocks, BLK_ROWS, depth), norm_gain[None, :], key_weight)

    placed = pl.pallas_call(
        place_kernel,
        out_shape=jax.ShapeDtypeStruct((blocks, BLK_ROWS, columns), jnp.bfloat16),
        in_specs=[in_smem, in_vmem],
        out_specs=any_space,
        scratch_shapes=[pltpu.SemaphoreType.DMA],
        compiler_params=pltpu.CompilerParams(vmem_limit_bytes=16 * MIB),
        name="place",
    )(slots, incoming.reshape(blocks, BLK_ROWS, columns))
    return placed.reshape(row_count, columns)


def solution(mesh):
    in_specs = (P("grp", "tp"), P(), P(None, "tp"), P())
    out_specs = P("grp", "tp")
    return jax.shard_map(
        functools.partial(on_device, mesh.shape["grp"], mesh.shape["tp"]),
        mesh=mesh, in_specs=in_specs, out_specs=out_specs, check_vma=False,
    )
```

```python
import functools

import jax
import jax.numpy as jnp
from jax import lax
from jax.experimental import pallas as pl
from jax.experimental.pallas import tpu as pltpu
from jax.sharding import PartitionSpec as P

BLK_ROWS = 8
EPS = 1e-05
MIB = 1024 * 1024
MESH = pl.DeviceIdType.MESH

NZ = 16
NY = 4
NX = 4
PER_Z = 4
SHIFTS = (3, 13, 4, 12, 5, 11, 1, 15, 2, 14, 6, 10, 7, 9, 8, 0)
STEPS = len(SHIFTS)
HOME_STEPS = 6
PIECES = 8
OTHER_CHUNK = 6
FIRST_HAND = (1, 2, 3, 4, 6, 7, 8, 9)
SECOND_HAND = (3, 4, 5, 6, 8, 9, 10, 12)
AHEAD = 2


def wrapped(v, n):
    return jnp.where(v >= n, v - n, v)


def core_served(x):
    return ((x + 1) // 2 + 1) % 2


def index_kernel(groups, table_ref, slot_ref, index_ref):
    me = lax.axis_index("grp")
    blocks = table_ref.shape[1]
    capacity = blocks // groups
    lane = lax.broadcasted_iota(jnp.int32, (groups, blocks), 1)
    row = lax.broadcasted_iota(jnp.int32, (groups, blocks), 0)

    def ranked(offset, value):
        chosen = (offset >= 0) & (offset < blocks)
        counted = chosen.astype(jnp.int32)
        shift = 1
        while shift < blocks:
            counted = counted + jnp.where(lane >= shift, pltpu.roll(counted, shift, 1), 0)
            shift *= 2
        result = jnp.zeros((groups, blocks), jnp.int32)
        for r in range(capacity):
            at_rank = jnp.where(chosen & (counted == r + 1), value, 0).astype(jnp.float32)
            found = jnp.sum(at_rank, axis=1, keepdims=True).astype(jnp.int32)
            result = jnp.where(lane == r, found, result)
        return result

    own = jnp.broadcast_to(table_ref[pl.ds(me, 1), :], (groups, blocks))
    index_ref[...] = ranked(own - row * blocks, lane)
    offset = table_ref[...] - me * blocks
    slot_ref[...] = ranked(offset, offset)


def place_kernel(slot_ref, in_ref, out_ref, sem):
    z = lax.axis_index("grp") // PER_Z
    for s in range(2):
        for j in range(STEPS):
            first = wrapped(z + (NZ - SHIFTS[j]) % NZ, NZ) * PER_Z + s
            for a in range(2):
                for r in range(2):
                    n = ((s * STEPS + j) * 2 + a) * 2 + r
                    slot = slot_ref[first + a * 2, r]
                    pltpu.make_async_copy(in_ref.at[n], out_ref.at[slot], sem).start()
    pltpu.make_async_copy(in_ref, out_ref, sem).wait()


def main_kernel(
    index_ref, rows_ref, gain_ref, weight_ref, out_ref,
    raw, away, gath, weight, other, keys, normed, gains,
    raw_sem, weight_sem, gain_sem, s_send, s_recv, z_send, z_recv, y_send, y_recv, f_send, f_recv,
    b_send, b_recv, a_send, a_recv, c_send, c_recv, k_send, k_recv, h_send, h_recv,
    token,
):
    g = lax.axis_index("grp")
    t = lax.axis_index("tp")
    z = g // PER_Z
    x_lo = (g // 2) % 2
    core = g % 2
    x_hi = t // NY
    y = t % NY
    x = x_lo + 2 * x_hi
    served = core_served(x)
    keeps = 1 - (served + core) % 2
    depth = rows_ref.shape[2]
    width = weight_ref.shape[0]
    parts = width // depth
    sub = 2 * BLK_ROWS
    chunk = 4 * sub
    half = 2 * STEPS * sub
    chunks = half // chunk
    home_chunks = HOME_STEPS // 2
    quarter = width // 4
    piece = quarter // PIECES

    def at_device(z_at, x_at, core_at):
        high = jnp.where(x_at >= 2, 1, 0)
        return {"grp": z_at * PER_Z + (x_at - 2 * high) * 2 + core_at, "tp": high * NY + y}

    a_peer = at_device(z, x + 1 - 2 * x_lo, core)
    b_peer = at_device(z, NX - 1 - x, core)
    c_peer = at_device(z, x, 1 - core)
    raw_copy = pltpu.make_async_copy(rows_ref, raw, raw_sem)
    raw_copy.start()

    y_up, y_down = wrapped(y + 1, NY), wrapped(y + NY - 1, NY)
    up = {"grp": g, "tp": x_hi * NY + y_up}
    down = {"grp": g, "tp": x_hi * NY + y_down}

    barrier = pltpu.get_barrier_semaphore()

    def signal(peer):
        pl.semaphore_signal(barrier, inc=1, device_id=peer, device_id_type=MESH)

    z_up = at_device(wrapped(z + 1, NZ), x, core)
    z_down = at_device(wrapped(z + NZ - 1, NZ), x, core)
    for peer in (up, down, z_up, z_down, c_peer):
        signal(peer)
    for m in range(1, NX):
        for k in range(2):
            signal(at_device(z, wrapped(x + m, NX), k))

    def origin(j):
        r, h = j // 2, j % 2
        return h * NY + (y, y_down, y_up, wrapped(y + 2, NY))[r]

    def weight_copy(j):
        return pltpu.make_async_copy(
            weight_ref.at[pl.ds(pl.multiple_of(origin(j) * depth, depth), depth)],
            weight.at[pl.ds(j * depth, depth)],
            weight_sem.at[j],
        )

    def gain_copy(j):
        return pltpu.make_async_copy(
            gain_ref.at[:, pl.ds(pl.multiple_of(origin(j) * depth, depth), depth)],
            gains.at[:, pl.ds(j * depth, depth)],
            gain_sem.at[j],
        )

    for j in range(parts):
        weight_copy(j).start()
    for j in range(parts):
        gain_copy(j).start()

    mine = [
        keeps * jnp.where((x_hi == m // 2) & (x_lo == m % 2), 1, 0) for m in range(4)
    ]
    stays = [
        keeps * jnp.where((core == n // 2) & (x_lo == 1 - n % 2), 1, 0) for n in range(4)
    ]
    last = STEPS - 1

    def s_copy(j, which):
        k = which * served + (1 - which) * (1 - served)
        return pltpu.make_async_remote_copy(
            src_ref=away.at[pl.ds(j * 4 + k * 2, 2)],
            dst_ref=gath.at[0, j, x_hi],
            send_sem=s_send.at[which, j],
            recv_sem=s_recv.at[which, j],
            device_id=(a_peer, b_peer)[which],
            device_id_type=MESH,
        )

    def s_arrival(j, which):
        return pltpu.make_async_remote_copy(
            src_ref=away.at[pl.ds(j * 4, 2)],
            dst_ref=gath.at[0, j, x_hi + which * (1 - 2 * x_hi)],
            send_sem=s_send.at[which, j],
            recv_sem=s_recv.at[which, j],
            device_id=(a_peer, b_peer)[which],
            device_id_type=MESH,
        )

    def z_copy(j, n):
        return pltpu.make_async_remote_copy(
            src_ref=away.at[j * 4 + n],
            dst_ref=gath.at[0, j, x_hi, x_lo],
            send_sem=z_send.at[j * 4 + n],
            recv_sem=z_recv.at[j * 4 + x_hi * 2 + x_lo],
            device_id=at_device(
                wrapped(z + SHIFTS[j], NZ), wrapped(2 * core + n % 2 + 1, NX), n // 2
            ),
            device_id_type=MESH,
        )

    def z_arrival(j, m):
        return pltpu.make_async_remote_copy(
            src_ref=away.at[j * 4 + m],
            dst_ref=gath.at[0, j, m // 2, m % 2],
            send_sem=z_send.at[j * 4 + m],
            recv_sem=z_recv.at[j * 4 + m],
            device_id=a_peer,
            device_id_type=MESH,
        )

    def y_copy(j, way):
        return pltpu.make_async_remote_copy(
            src_ref=gath.at[0, j],
            dst_ref=gath.at[1 + way, j],
            send_sem=y_send.at[way, j],
            recv_sem=y_recv.at[way, j],
            device_id=(up, down)[way],
            device_id_type=MESH,
        )

    def f_copy(j, way):
        return pltpu.make_async_remote_copy(
            src_ref=gath.at[1 + way, j, way],
            dst_ref=gath.at[3, j, way],
            send_sem=f_send.at[way, j],
            recv_sem=f_recv.at[way, j],
            device_id=(up, down)[way],
            device_id_type=MESH,
        )

    def piece_of(q, p):
        return pl.ds(pl.multiple_of(q * quarter + p * piece, piece), piece)

    def b_copy(p):
        at = piece_of((1 - x_lo) * 2 + core, p)
        return pltpu.make_async_remote_copy(
            src_ref=weight.at[at], dst_ref=other.at[at],
            send_sem=b_send.at[p], recv_sem=b_recv.at[p],
            device_id=b_peer, device_id_type=MESH,
        )

    def b_arrival(p):
        at = piece_of(x_lo * 2 + core, p)
        return pltpu.make_async_remote_copy(
            src_ref=weight.at[at], dst_ref=other.at[at],
            send_sem=b_send.at[p], recv_sem=b_recv.at[p],
            device_id=b_peer, device_id_type=MESH,
        )

    def a_copy(p, side):
        at = piece_of((x_lo + side * (1 - 2 * x_lo)) * 2 + core, p)
        return pltpu.make_async_remote_copy(
            src_ref=other.at[at], dst_ref=other.at[at],
            send_sem=a_send.at[p], recv_sem=a_recv.at[p],
            device_id=a_peer, device_id_type=MESH,
        )

    def c_copy(p, late, at_core):
        at = piece_of((x_lo + late * (1 - 2 * x_lo)) * 2 + at_core, p)
        return pltpu.make_async_remote_copy(
            src_ref=other.at[at], dst_ref=other.at[at],
            send_sem=c_send.at[late, p], recv_sem=c_recv.at[late, p],
            device_id=c_peer, device_id_type=MESH,
        )

    def rows_of(i):
        return pl.ds(pl.multiple_of(i * chunk, chunk), chunk)

    def k_copy(i, which, source):
        return pltpu.make_async_remote_copy(
            src_ref=keys.at[which, rows_of(i)],
            dst_ref=out_ref.at[pl.ds(pl.multiple_of(source * half + i * chunk, chunk), chunk)],
            send_sem=k_send.at[which, i],
            recv_sem=k_recv.at[which, i],
            device_id=(a_peer, b_peer)[which],
            device_id_type=MESH,
        )

    def h_copy(n, which):
        side = x_hi + which * (1 - 2 * x_hi)
        at = (core * STEPS + n // 2) * 2 + 1 - x_lo
        return pltpu.make_async_remote_copy(
            src_ref=keys.at[which, pl.ds(pl.multiple_of(n * sub, sub), sub)],
            dst_ref=out_ref.at[pl.ds(pl.multiple_of(at * sub, sub), sub)],
            send_sem=h_send.at[which, n],
            recv_sem=h_recv.at[core, n // 2 * 2 + 1 - x_lo],
            device_id=at_device(wrapped(z + SHIFTS[n // 2], NZ), n % 2 + 2 * side, served),
            device_id_type=MESH,
        )

    def h_arrival(n, s):
        return pltpu.make_async_remote_copy(
            src_ref=keys.at[0, pl.ds(pl.multiple_of(n * sub, sub), sub)],
            dst_ref=out_ref.at[pl.ds(pl.multiple_of((s * STEPS * 2 + n) * sub, sub), sub)],
            send_sem=h_send.at[0, n],
            recv_sem=h_recv.at[s, n],
            device_id=a_peer,
            device_id_type=MESH,
        )

    def arrange(j):
        to_z = wrapped(z + SHIFTS[j], NZ) * PER_Z
        for n in range(4):
            to = to_z + (n % 2) * 2 + n // 2
            first = raw[index_ref[to, 0]]
            second = raw[index_ref[to, 1]]
            away[j * 4 + n, 0] = first
            away[j * 4 + n, 1] = second
            if j == last:
                @pl.when(stays[n] > 0)
                def _():
                    gath[0, j, x_hi, x_lo, 0] = first
                    gath[0, j, x_hi, x_lo, 1] = second

    raw_copy.wait()
    for j in range(STEPS):
        arrange(j)
    pl.semaphore_wait(barrier, 5 + 2 * (NX - 1))
    for j in range(HOME_STEPS):
        for which in range(2):
            s_copy(j, which).start()

    def send_rows(shift):
        j = SHIFTS.index(shift)
        for n in range(4):
            if j == last:
                @pl.when(stays[n] < 1)
                def _():
                    z_copy(j, n).start()
            else:
                z_copy(j, n).start()

    def start_ring(j):
        for way in range(2):
            y_copy(j, way).start()

    def start_home(j):
        for which in range(2):
            s_arrival(j, which).wait_recv()
        start_ring(j)

    for d in range(1, NZ // 2 + 1):
        ways = 2 if d < NZ // 2 else 1
        for way in range(ways):
            pl.semaphore_signal(
                token.at[way, d - 1], inc=1, device_id=(z_up, z_down)[way], device_id_type=MESH
            )
        if d == 1:
            send_rows(0)
            for j in range(parts):
                weight_copy(j).wait()
            for p in range(PIECES):
                b_copy(p).start()
        for way in range(ways):
            pl.semaphore_wait(token.at[way, d - 1], 1)
        for shift in sorted({d, NZ - d}):
            if shift in SHIFTS[HOME_STEPS:]:
                send_rows(shift)
        if d == 5:
            start_home(0)
            start_home(1)
        if d == 7:
            start_home(2)
            start_home(3)
    for j in range(4, HOME_STEPS):
        start_home(j)
    for j in range(parts):
        gain_copy(j).wait()

    sub = 2 * BLK_ROWS

    def normalise(i):
        def norm_rows(n, carry):
            to = pl.ds(pl.multiple_of(i * chunk + n * sub, sub), sub)

            def values(j):
                held = gath[j // 2, i * 2 + n // 2, j % 2, n - n // 2 * 2]
                return held.astype(jnp.float32).reshape(sub, depth)

            row_sum = 0.0
            row_sq = 0.0
            for j in range(parts):
                v = values(j)
                row_sum = row_sum + jnp.sum(v, axis=1, keepdims=True)
                row_sq = row_sq + jnp.sum(v * v, axis=1, keepdims=True)
            mean = row_sum / width
            scale = lax.rsqrt(row_sq / width - mean * mean + EPS)
            for j in range(parts):
                cols = pl.ds(j * depth, depth)
                normed[to, cols] = ((values(j) - mean) * scale * gains[:, cols]).astype(
                    jnp.bfloat16
                )
            return carry

        lax.fori_loop(0, chunk // sub, norm_rows, 0)

    def project(start, count, which):
        at = pl.ds(pl.multiple_of(start, chunk), count)
        keys[which, at, :] = jnp.dot(
            normed[at, :], (weight, other)[which][...], preferred_element_type=jnp.float32
        ).astype(jnp.bfloat16)

    def rows_arrived(i, e):
        for m in range(4):
            if e == last % 2:
                @pl.when((i < chunks - 1) | (mine[m] < 1))
                def _():
                    z_arrival(i * 2 + e, m).wait_recv()
            else:
                z_arrival(i * 2 + e, m).wait_recv()

    def forward(j):
        for way in range(2):
            y_copy(j, way).wait_recv()
            f_copy(j, way).start()

    def step(i, carry):
        for e in range(2):
            @pl.when(i < chunks)
            def _():
                forward(i * 2 + e)

            @pl.when((i + AHEAD >= home_chunks) & (i + AHEAD < chunks))
            def _():
                rows_arrived(i + AHEAD, e)
                start_ring((i + AHEAD) * 2 + e)

            for p in range(PIECES):
                if FIRST_HAND[p] % 2 == e:
                    @pl.when(i == FIRST_HAND[p] // 2)
                    def _():
                        b_arrival(p).wait_recv()
                        a_copy(p, 0).start()
                        c_copy(p, 0, core).start()

            for p in range(PIECES):
                if SECOND_HAND[p] % 2 == e:
                    @pl.when(i == SECOND_HAND[p] // 2)
                    def _():
                        a_copy(p, 1).wait_recv()
                        c_copy(p, 1, core).start()

        @pl.when(i > 0)
        def _():
            c = i - 1
            for e in range(2):
                for way in range(2):
                    f_copy(c * 2 + e, way).wait_recv()
            normalise(c)
            project(c * chunk, chunk, 0)

            for home in range(home_chunks):
                @pl.when(c == home)
                def _():
                    for n in range(home * 4, home * 4 + 4):
                        h_copy(n, 0).start()

            @pl.when(c >= home_chunks)
            def _():
                k_copy(c, 0, served).start()

        @pl.when(i == OTHER_CHUNK)
        def _():
            for p in range(PIECES):
                for late in range(2):
                    c_copy(p, late, 1 - core).wait_recv()
            project(0, home_chunks * chunk, 1)
            for n in range(home_chunks * 4):
                h_copy(n, 1).start()
            project(home_chunks * chunk, (OTHER_CHUNK - home_chunks) * chunk, 1)
            for c in range(home_chunks, OTHER_CHUNK):
                k_copy(c, 1, served).start()

        @pl.when(i > OTHER_CHUNK)
        def _():
            project((i - 1) * chunk, chunk, 1)
            k_copy(i - 1, 1, served).start()

        return carry

    lax.fori_loop(0, chunks + 1, step, 0)

    for j in range(HOME_STEPS, STEPS):
        for n in range(4):
            if j == last:
                @pl.when(stays[n] < 1)
                def _():
                    z_copy(j, n).wait_send()
            else:
                z_copy(j, n).wait_send()

    def home_sent(j, carry):
        for which in range(2):
            s_copy(j, which).wait_send()
        return carry

    def ring_sent(j, carry):
        for way in range(2):
            y_copy(j, way).wait_send()
            f_copy(j, way).wait_send()
        return carry

    def weight_sent(p, carry):
        b_copy(p).wait_send()
        a_copy(p, 0).wait_send()
        for late in range(2):
            c_copy(p, late, core).wait_send()
        return carry

    def keys_done(i, carry):
        for which in range(2):
            k_copy(i, which, served).wait_send()
            k_copy(i, which, served + (1 - which) * (1 - 2 * served)).wait_recv()
        return carry

    for n in range(HOME_STEPS * 2):
        for which in range(2):
            h_copy(n, which).wait_send()
            h_arrival(n, which).wait_recv()
    lax.fori_loop(0, HOME_STEPS, home_sent, 0)
    lax.fori_loop(0, STEPS, ring_sent, 0)
    lax.fori_loop(0, PIECES, weight_sent, 0)
    lax.fori_loop(home_chunks, chunks, keys_done, 0)


def on_device(groups, parts, memory_rows, norm_gain, key_weight, owner_table):
    row_count, depth = memory_rows.shape
    columns = key_weight.shape[1]
    blocks = row_count // BLK_ROWS
    any_space = pl.BlockSpec(memory_space=pl.ANY)
    in_hbm = pl.BlockSpec(memory_space=pltpu.HBM)
    in_vmem = pl.BlockSpec(memory_space=pltpu.VMEM)
    in_smem = pl.BlockSpec(memory_space=pltpu.SMEM)

    dma = pltpu.SemaphoreType.DMA
    listing = jax.ShapeDtypeStruct((groups, blocks), jnp.int32)
    slots, index = pl.pallas_call(
        functools.partial(index_kernel, groups),
        out_shape=[listing, listing],
        in_specs=[in_vmem],
        out_specs=[in_vmem, in_vmem],
        compiler_params=pltpu.CompilerParams(vmem_limit_bytes=4 * MIB),
        name="index",
    )(owner_table.reshape(groups, blocks))

    chunks = blocks // 16
    incoming = pl.pallas_call(
        main_kernel,
        out_shape=jax.ShapeDtypeStruct((row_count, columns), jnp.bfloat16),
        in_specs=[in_smem, in_hbm, in_hbm, in_hbm],
        out_specs=any_space,
        scratch_shapes=[
            pltpu.VMEM((blocks, BLK_ROWS, depth), jnp.bfloat16),
            pltpu.VMEM((STEPS * 4, 2, BLK_ROWS, depth), jnp.bfloat16),
            pltpu.VMEM((NY, STEPS, 2, 2, 2, BLK_ROWS, depth), jnp.bfloat16),
            pltpu.VMEM((depth * parts, columns), jnp.bfloat16),
            pltpu.VMEM((depth * parts, columns), jnp.bfloat16),
            pltpu.VMEM((2, row_count // 2, columns), jnp.bfloat16),
            pltpu.VMEM((row_count // 2, depth * parts), jnp.bfloat16),
            pltpu.VMEM((1, depth * parts), jnp.float32),
            dma,
            dma((parts,)),
            dma((parts,)),
            dma((2, HOME_STEPS)),
            dma((2, HOME_STEPS)),
            dma((STEPS * 4,)),
            dma((STEPS * 4,)),
            dma((2, STEPS)),
            dma((2, STEPS)),
            dma((2, STEPS)),
            dma((2, STEPS)),
            dma((PIECES,)),
            dma((PIECES,)),
            dma((PIECES,)),
            dma((PIECES,)),
            dma((2, PIECES)),
            dma((2, PIECES)),
            dma((2, chunks)),
            dma((2, chunks)),
            dma((2, HOME_STEPS * 2)),
            dma((2, HOME_STEPS * 2)),
            pltpu.SemaphoreType.REGULAR((2, NZ // 2)),
        ],
        compiler_params=pltpu.CompilerParams(
            collective_id=0, has_side_effects=True, vmem_limit_bytes=52 * MIB
        ),
        name="exchange",
    )(index, memory_rows.reshape(blocks, BLK_ROWS, depth), norm_gain[None, :], key_weight)

    placed = pl.pallas_call(
        place_kernel,
        out_shape=jax.ShapeDtypeStruct((blocks, BLK_ROWS, columns), jnp.bfloat16),
        in_specs=[in_smem, in_vmem],
        out_specs=any_space,
        scratch_shapes=[pltpu.SemaphoreType.DMA],
        compiler_params=pltpu.CompilerParams(vmem_limit_bytes=16 * MIB),
        name="place",
    )(slots, incoming.reshape(blocks, BLK_ROWS, columns))
    return placed.reshape(row_count, columns)


def solution(mesh):
    in_specs = (P("grp", "tp"), P(), P(None, "tp"), P())
    out_specs = P("grp", "tp")
    return jax.shard_map(
        functools.partial(on_device, mesh.shape["grp"], mesh.shape["tp"]),
        mesh=mesh, in_specs=in_specs, out_specs=out_specs, check_vma=False,
    )
```
